32 devices in a mesh: dp: 8 (over y, x, core), fsdp: 4 (over z).
Axes of the slice: x: 2, y: 2, z: 4, core: 2. Of those that a mesh axis runs over, the one named last changes fastest.
Arguments:
- inputs: bfloat16 [32768, 768], P(('dp', 'fsdp')), may hold values from -6 to 6
- segment_ids: int32 [32, 1024], P(('dp', 'fsdp')), may hold values from 0 to 7, never falling along the last dimension, each value on 1 to 256 neighbouring positions
- cotangent: bfloat16 [32768, 768], P(('dp', 'fsdp')), may hold values from -6 to 6
- ln1_gain: float32 [768], P(('dp', 'fsdp')), may hold values from 0.5 to 1.5
- ln1_bias: float32 [768], P(('dp', 'fsdp')), may hold values from -1.75 to 1.75
- w_query: float32 [768, 768], P(('dp', 'fsdp')), may hold values from -0.3125 to 0.3125
- b_query: float32 [768], P(('dp', 'fsdp')), may hold values from -1.75 to 1.75
- w_key: float32 [768, 768], P(('dp', 'fsdp')), may hold values from -0.3125 to 0.3125
- w_value: float32 [768, 768], P(('dp', 'fsdp')), may hold values from -0.21875 to 0.21875
- b_value: float32 [768], P(('dp', 'fsdp')), may hold values from -1.75 to 1.75
- w_out: float32 [768, 768], P(('dp', 'fsdp')), may hold values from -0.875 to 0.875
- b_out: float32 [768], P(('dp', 'fsdp')), may hold values from -1.75 to 1.75
- ln2_gain: float32 [768], P(('dp', 'fsdp')), may hold values from 0.5 to 1.5
- ln2_bias: float32 [768], P(('dp', 'fsdp')), may hold values from -1.75 to 1.75
- w_up: float32 [768, 3072], P(('dp', 'fsdp')), may hold values from -0.21875 to 0.21875
- b_up: float32 [3072], P(('dp', 'fsdp')), may hold values from -1.75 to 1.75
- w_down: float32 [3072, 768], P(('dp', 'fsdp')), may hold values from -0.109375 to 0.109375
- b_down: float32 [768], P(('dp', 'fsdp')), may hold values from -1.75 to 1.75
Outputs:
- block_output: bfloat16 [32768, 768], P(('dp', 'fsdp'))
- input_grad: float32 [32768, 768], P(('dp', 'fsdp'))
- grad_ln1_gain: float32 [768], P(('dp', 'fsdp'))
- grad_ln1_bias: float32 [768], P(('dp', 'fsdp'))
- grad_w_query: float32 [768, 768], P(('dp', 'fsdp'))
- grad_b_query: float32 [768], P(('dp', 'fsdp'))
- grad_w_key: float32 [768, 768], P(('dp', 'fsdp'))
- grad_w_value: float32 [768, 768], P(('dp', 'fsdp'))
- grad_b_value: float32 [768], P(('dp', 'fsdp'))
- grad_w_out: float32 [768, 768], P(('dp', 'fsdp'))
- grad_b_out: float32 [768], P(('dp', 'fsdp'))
- grad_ln2_gain: float32 [768], P(('dp', 'fsdp'))
- grad_ln2_bias: float32 [768], P(('dp', 'fsdp'))
- grad_w_up: float32 [768, 3072], P(('dp', 'fsdp'))
- grad_b_up: float32 [3072], P(('dp', 'fsdp'))
- grad_w_down: float32 [3072, 768], P(('dp', 'fsdp'))
- grad_b_down: float32 [768], P(('dp', 'fsdp'))
The draws below stay inside these ranges and needn't reach their ends.
Inputs may be any that keep to these rules, and one draw needn't show every extreme that they name: `segment_ids`: each row of 1024 tokens holds 8 documents numbered 0 to 7 in order, never falling, each 1 to 256 tokens long, one of exactly 256.
All inputs are finite; a program needn't handle non-finite values.
Results may differ from the reference program's by a relative error of at most 0.013.
The reference program's roundings to bfloat16 on the way count: a program that leaves them out, or rounds other values in their place, can miss the bound.
Values may be sent and summed in bfloat16 or wider, within the bound.
A program may use at most 320 MiB of HBM per device.

```python
import math
import jax
import jax.numpy as jnp
import numpy as np
from jax import lax

D = 768
HEADS = 12
HEAD = 64
FF = 3072
SEQ_LEN = 1024
SEQS = 32
TOKENS = 32768


def spiked(values, rng, source, target, parts, factor):
    def block_of(axis_at):
        return (jnp.arange(values.shape[axis_at]) // (values.shape[axis_at] // parts)).reshape((-1,) + (1,) * (values.ndim - 1 - axis_at))

    one_side = jax.random.permutation(rng, parts)[block_of(target)]
    second = (block_of(target) + parts // 2) % parts
    return jnp.where((block_of(source) == one_side) | (block_of(source) == second), factor * values, values)


def block_scale(rng, dims, cuts, least, high):
    factor_of, own = 1.0, jax.random.fold_in(rng, 6)
    for position, shards_of in cuts:
        draws = jnp.exp(jax.random.uniform(jax.random.fold_in(own, position), (shards_of,), jnp.float32, least / len(cuts), high / len(cuts)))
        factor_of = factor_of * jnp.repeat(draws, dims[position] // shards_of).reshape([-1 if axis == position else 1 for axis in range(len(dims))])
    return factor_of


def length_profile(count, total, most, lean):
    portions = [(1 << 20) // math.isqrt(rank ** lean) + 1 for rank in range(2, count + 1)]
    rest, holding = total - most - (count - 1), [1] * (count - 1)
    while rest > 0:
        free = [i for i in range(count - 1) if holding[i] < most]
        pool, budget = sum([portions[i] for i in free]), rest
        for i in free:
            extra = min(most - holding[i], max(1, budget * portions[i] // pool), rest)
            holding[i] = holding[i] + extra
            rest = rest - extra
    return np.array([most] + holding)


def ragged_sizes(own_key, number_of, total, most, slope):
    if number_of == 2:
        one = jax.random.randint(own_key, (), max(1, total - most), min(most, total - 1) + 1)
        return jnp.stack([one, total - one])
    sizes = jnp.asarray(length_profile(number_of, total, most, slope), jnp.int32)
    pairs = (number_of - 1) // 2
    source_of, sink = sizes[1:1 + 2 * pairs:2], sizes[2:2 + 2 * pairs:2]
    room = jnp.minimum(source_of - 1, most - sink)
    shifted = jax.random.randint(jax.random.fold_in(own_key, 1), (pairs,), 0, 1 << 20) % (room + 1)
    sizes = sizes.at[1:1 + 2 * pairs:2].set(source_of - shifted).at[2:2 + 2 * pairs:2].set(sink + shifted)
    return sizes[jax.random.permutation(jax.random.fold_in(own_key, 2), number_of)]


def gaussian(key, extent, scale, most, split=(), kind=jnp.bfloat16):
    array = scale * jax.random.normal(key, extent, jnp.float32)
    if split:
        array = array * block_scale(key, extent, split, -0.22, 0.18)
    return jnp.clip(array, -most, most).astype(kind)


def bell_draw_with(key, dims, scale, limit, pieces, heavy, dtype=jnp.bfloat16):
    values = scale * jax.random.normal(key, dims, jnp.float32)
    if pieces:
        values = values * block_scale(key, dims, pieces, -0.22, 0.18)
    return jnp.clip(spiked(values, jax.random.fold_in(key, 3), *heavy), -limit, limit).astype(dtype)


def setup_inputs(seed: int = 0) -> dict:
    key_of = jax.random.split(jax.random.key(seed), 19)
    inputs = gaussian(key_of[0], (TOKENS, D), 1.0, 6.0, ((0, 32),))
    segment_ids = jax.vmap(lambda own: jnp.searchsorted(jnp.cumsum(ragged_sizes(own, 8, SEQ_LEN, SEQ_LEN // 4, 2)), jnp.arange(SEQ_LEN), side="right"))(jax.random.split(key_of[1], SEQS)).reshape((SEQS, SEQ_LEN)).astype(jnp.int32)
    cotangent = bell_draw_with(key_of[2], (TOKENS, D), 1.0, 6.0, ((0, 32),), (0, 1, 32, 2.75))
    ln1_gain = jnp.clip(1.0 + 0.1 * jax.random.normal(key_of[3], (D,), jnp.float32), 0.5, 1.5)
    ln1_bias = gaussian(key_of[4], (D,), 0.3, 1.75, ((0, 32),), jnp.float32)
    w_query = gaussian(key_of[5], (D, D), (D // 2) ** -0.5, 0.3125, ((0, 32),), jnp.float32)
    b_query = gaussian(key_of[6], (D,), 0.3, 1.75, ((0, 32),), jnp.float32)
    w_key = gaussian(key_of[7], (D, D), (D // 2) ** -0.5, 0.3125, ((0, 32),), jnp.float32)
    w_value = gaussian(key_of[8], (D, D), D ** -0.5, 0.21875, ((0, 32),), jnp.float32)
    b_value = gaussian(key_of[9], (D,), 0.3, 1.75, ((0, 32),), jnp.float32)
    w_out = gaussian(key_of[10], (D, D), (D // 16) ** -0.5, 0.875, ((0, 32),), jnp.float32)
    b_out = gaussian(key_of[11], (D,), 0.3, 1.75, ((0, 32),), jnp.float32)
    ln2_gain = jnp.clip(1.0 + 0.1 * jax.random.normal(key_of[12], (D,), jnp.float32), 0.5, 1.5)
    ln2_bias = gaussian(key_of[13], (D,), 0.3, 1.75, ((0, 32),), jnp.float32)
    w_up = gaussian(key_of[14], (D, FF), D ** -0.5, 0.21875, ((0, 32),), jnp.float32)
    b_up = gaussian(key_of[15], (FF,), 0.3, 1.75, ((0, 32),), jnp.float32)
    w_down = gaussian(key_of[16], (FF, D), FF ** -0.5, 0.109375, ((0, 32),), jnp.float32)
    b_down = gaussian(key_of[17], (D,), 0.3, 1.75, ((0, 32),), jnp.float32)
    return dict(inputs=inputs, segment_ids=segment_ids, cotangent=cotangent, ln1_gain=ln1_gain, ln1_bias=ln1_bias, w_query=w_query, b_query=b_query, w_key=w_key, w_value=w_value, b_value=b_value, w_out=w_out, b_out=b_out, ln2_gain=ln2_gain, ln2_bias=ln2_bias, w_up=w_up, b_up=b_up, w_down=w_down, b_down=b_down)


@jax.custom_vjp
def low(v):
    return lax.optimization_barrier(v.astype(jnp.bfloat16)).astype(jnp.float32)

@jax.custom_vjp
def low_back(v):
    return v

def low_keep(v):
    return (low(v), None)

def low_pass(kept, grad):
    return (grad,)

def back_keep(v):
    return (v, None)

def back_low(kept, grad):
    return (low(grad),)
low.defvjp(low_keep, low_pass)
low_back.defvjp(back_keep, back_low)
NORM_EPSILON = 1e-12
MASK_VALUE = -1e+30

def layer_norm(vector_rows, gain_row, bias_row):
    centre = vector_rows - lax.optimization_barrier(jnp.mean(vector_rows, axis=-1, keepdims=True))
    spread = lax.optimization_barrier(jnp.mean(centre * centre, axis=-1, keepdims=True))
    return centre * lax.rsqrt(spread + NORM_EPSILON) * gain_row + bias_row

def matmul(left_arg, right_arg):
    return jnp.dot(left_arg, right_arg, precision=lax.Precision.HIGHEST, preferred_element_type=jnp.float32)

def sequence_forward(rounded, tokens_seq, segments):
    ln1_gain, ln1_bias, w_query, b_query, w_key, w_value, b_value, w_out, b_out, ln2_gain, ln2_bias, w_up, b_up, w_down, b_down = rounded
    length = tokens_seq.shape[0]
    normed_one = low(layer_norm(tokens_seq, ln1_gain, ln1_bias))
    queries = low_back(low(matmul(normed_one, w_query) + b_query)).reshape(length, HEADS, HEAD)
    key_rows = low_back(low(matmul(normed_one, w_key))).reshape(length, HEADS, HEAD)
    values = low_back(low(matmul(normed_one, w_value) + b_value)).reshape(length, HEADS, HEAD)
    scores = low_back(jnp.einsum('qhe,khe->hqk', queries, key_rows, precision=lax.Precision.HIGHEST) * 0.125)
    same_doc = segments[:, None] == segments[None, :]
    scores = jnp.where(same_doc[None, :, :], scores, MASK_VALUE)
    prob_rows = low(jax.nn.softmax(scores, axis=-1))
    mixed = jnp.einsum('hqk,khe->qhe', prob_rows, values, precision=lax.Precision.HIGHEST).reshape(length, HEADS * HEAD)
    mixed = low_back(low(mixed))
    hidden_one = tokens_seq + low_back(matmul(mixed, w_out) + b_out)
    normed_two = low(layer_norm(hidden_one, ln2_gain, ln2_bias))
    up_rows = low_back(matmul(normed_two, w_up) + b_up)
    activated = low(jax.nn.gelu(up_rows, approximate=False))
    return hidden_one + low_back(matmul(activated, w_down) + b_down)

def reference(inputs, segment_ids, cotangent, ln1_gain, ln1_bias, w_query, b_query, w_key, w_value, b_value, w_out, b_out, ln2_gain, ln2_bias, w_up, b_up, w_down, b_down):
    params = (ln1_gain, ln1_bias, w_query, b_query, w_key, w_value, b_value, w_out, b_out, ln2_gain, ln2_bias, w_up, b_up, w_down, b_down)
    sequences = inputs.astype(jnp.float32).reshape(SEQS, SEQ_LEN, D)

    def whole_block(param_set, token_set):
        rounded = tuple((low(weight_entry) for weight_entry in param_set))

        def one_sequence(seq_pair):
            return sequence_forward(rounded, seq_pair[0], seq_pair[1])
        return lax.map(jax.checkpoint(one_sequence), (token_set, segment_ids))
    result, pullback = jax.vjp(whole_block, params, sequences)
    weight_grads, input_grad = pullback(cotangent.astype(jnp.float32).reshape(SEQS, SEQ_LEN, D))
    return (result.reshape(TOKENS, D).astype(jnp.bfloat16), input_grad.reshape(TOKENS, D), weight_grads[0], weight_grads[1], weight_grads[2], weight_grads[3], weight_grads[4], weight_grads[5], weight_grads[6], weight_grads[7], weight_grads[8], weight_grads[9], weight_grads[10], weight_grads[11], weight_grads[12], weight_grads[13], weight_grads[14])
```

```python
import functools

import jax
import jax.numpy as jnp
from jax import lax
from jax.experimental import pallas as pl
from jax.experimental.pallas import tpu as pltpu
from jax.sharding import PartitionSpec as P

HEAD = 64
LANES = 128
QBLOCK = 256
DOC_MAX = 256
NORM_EPSILON = 1e-12
MASK_VALUE = -1e30
AXES = ("dp", "fsdp")
F32 = jnp.float32
BF16 = jnp.bfloat16
VMEM_BYTES = 66_000_000


def mm(a, b, ca, cb):
    return lax.dot_general(a, b, (((ca,), (cb,)), ((), ())), preferred_element_type=F32)


def window(i, length):
    lo = max(0, i * QBLOCK - DOC_MAX)
    hi = min(length, (i + 1) * QBLOCK + DOC_MAX)
    return lo, hi


def norm_parts(v):
    centre = v - jnp.mean(v, axis=-1, keepdims=True)
    spread = jnp.mean(centre * centre, axis=-1, keepdims=True)
    rstd = lax.rsqrt(spread + NORM_EPSILON)
    return centre * rstd, rstd


def fill_bias(segc_ref, segr_ref, bias_ref, length):
    at = 0
    for i in range(length // QBLOCK):
        lo, hi = window(i, length)
        same = segc_ref[lo:hi, :] == segr_ref[:, i * QBLOCK : (i + 1) * QBLOCK]
        bias_ref[at : at + hi - lo, :] = jnp.where(same, 0.0, MASK_VALUE)
        at += hi - lo


def bias_rows(length):
    return sum(window(i, length)[1] - window(i, length)[0] for i in range(length // QBLOCK))


def lane_mask(h):
    lane = lax.broadcasted_iota(jnp.int32, (1, LANES), 1)
    return jnp.where(lax.div(lane, HEAD) == h, 1.0, 0.0)


def attn_fwd_kernel(
    x_ref, wq_ref, wk_ref, wv_ref, vec_ref, bq_ref, bv_ref, segc_ref, segr_ref,
    q_ref, k_ref, v_ref, o_ref, lse_ref, n1_ref, bias_ref, vt_ref,
):
    length = x_ref.shape[0]

    @pl.when(pl.program_id(0) == 0)
    def _():
        xhat, _ = norm_parts(x_ref[...].astype(F32))
        n1_ref[...] = (xhat * vec_ref[0:1, :] + vec_ref[1:2, :]).astype(BF16)
        fill_bias(segc_ref, segr_ref, bias_ref, length)

    n1 = n1_ref[...]
    q_ref[...] = (mm(n1, wq_ref[...], 1, 0) + bq_ref[...]).astype(BF16)
    k_ref[...] = mm(n1, wk_ref[...], 1, 0).astype(BF16)
    v_ref[...] = (mm(n1, wv_ref[...], 1, 0) + bv_ref[...]).astype(BF16)

    def pair(pp, carry):
        cols = pl.ds(pl.multiple_of(pp * LANES, LANES), LANES)
        vt_ref[...] = v_ref[:, cols].T
        at = 0
        for i in range(length // QBLOCK):
            lo, hi = window(i, length)
            rows = slice(i * QBLOCK, (i + 1) * QBLOCK)
            kk = k_ref[lo:hi, cols]
            qq = q_ref[rows, cols].astype(F32) * 0.125
            outs = []
            for h in range(2):
                qm = (qq * lane_mask(h)).astype(BF16)
                s = mm(kk, qm, 1, 1) + bias_ref[at : at + hi - lo, :]
                top = jnp.max(s, axis=0, keepdims=True)
                e = jnp.exp(s - top)
                total = jnp.sum(e, axis=0, keepdims=True)
                pr = (e * (1.0 / total)).astype(BF16)
                outs.append(mm(vt_ref[h * HEAD : (h + 1) * HEAD, lo:hi], pr, 1, 0))
                lse_ref[pp * 2 + h, :, rows] = top + jnp.log(total)
            o_ref[rows, cols] = jnp.concatenate(outs, axis=0).T.astype(BF16)
            at += hi - lo
        return carry

    lax.fori_loop(0, q_ref.shape[1] // LANES, pair, 0)


def full(shape):
    return pl.BlockSpec(shape, lambda *g: (0,) * len(shape), pipeline_mode=pl.Buffered(1))


def attention_forward(x, w_qkv, rows_vec, segc, segr, ):
    length, width = x.shape
    group = 2 * LANES
    steps = width // group
    heads = width // HEAD
    col = pl.BlockSpec((length, group), lambda p: (0, p))
    return pl.pallas_call(
        attn_fwd_kernel,
        grid=(steps,),
        in_specs=[
            full((length, width)),
            pl.BlockSpec((width, group), lambda p: (0, p)),
            pl.BlockSpec((width, group), lambda p: (0, steps + p)),
            pl.BlockSpec((width, group), lambda p: (0, 2 * steps + p)),
            full(rows_vec.shape),
            pl.BlockSpec((1, group), lambda p: (0, p)),
            pl.BlockSpec((1, group), lambda p: (0, p)),
            full((length, 1)),
            full((1, length)),
        ],
        out_specs=[col, col, col, col, pl.BlockSpec((group // HEAD, 1, length), lambda p: (p, 0, 0)),
                   pl.BlockSpec((length, width), lambda p: (0, 0))],
        out_shape=[jax.ShapeDtypeStruct((length, width), BF16)] * 4
        + [jax.ShapeDtypeStruct((heads, 1, length), F32), jax.ShapeDtypeStruct((length, width), BF16)],
        scratch_shapes=[
            pltpu.VMEM((bias_rows(length), QBLOCK), F32),
            pltpu.VMEM((LANES, length), BF16),
        ],
        compiler_params=pltpu.CompilerParams(vmem_limit_bytes=VMEM_BYTES),
        name="attn_fwd",
    )(x, w_qkv, w_qkv, w_qkv, rows_vec, rows_vec[2:3], rows_vec[3:4], segc, segr)


def attn_bwd_kernel(
    q_ref, k_ref, v_ref, g_ref, lse_ref, segc_ref, segr_ref,
    dq_ref, dk_ref, dv_ref, bias_ref, kt_ref, dk_acc, dv_acc,
):
    length = q_ref.shape[0]

    @pl.when(pl.program_id(0) == 0)
    def _():
        fill_bias(segc_ref, segr_ref, bias_ref, length)

    kt_ref[...] = k_ref[...].T
    dk_acc[...] = jnp.zeros_like(dk_acc)
    dv_acc[...] = jnp.zeros_like(dv_acc)
    at = 0
    for i in range(length // QBLOCK):
        lo, hi = window(i, length)
        rows = slice(i * QBLOCK, (i + 1) * QBLOCK)
        kk = k_ref[lo:hi, :]
        vv = v_ref[lo:hi, :]
        qq = q_ref[rows, :].astype(F32) * 0.125
        gg = g_ref[rows, :].astype(F32)
        outs = []
        dk_sum = dv_sum = None
        for h in range(2):
            keep = lane_mask(h)
            qm = (qq * keep).astype(BF16)
            gm = (gg * keep).astype(BF16)
            s = mm(kk, qm, 1, 1) + bias_ref[at : at + hi - lo, :]
            pr = jnp.exp(s - lse_ref[h, :, rows])
            gp = mm(vv, gm, 1, 1)
            centre = jnp.sum(pr * gp, axis=0, keepdims=True)
            gs = (pr * (gp - centre)).astype(BF16)
            dv = mm(pr.astype(BF16), gm, 1, 0)
            dk = mm(gs, qm, 1, 0)
            dk_sum = dk if dk_sum is None else dk_sum + dk
            dv_sum = dv if dv_sum is None else dv_sum + dv
            outs.append(mm(kt_ref[h * HEAD : (h + 1) * HEAD, lo:hi], gs, 1, 0))
        dk_acc[lo:hi, :] += dk_sum
        dv_acc[lo:hi, :] += dv_sum
        dq_ref[rows, :] = (jnp.concatenate(outs, axis=0).T * 0.125).astype(BF16)
        at += hi - lo
    dk_ref[...] = dk_acc[...].astype(BF16)
    dv_ref[...] = dv_acc[...].astype(BF16)


def attention_backward(q, k, v, g, lse, segc, segr):
    length, width = q.shape
    col = pl.BlockSpec((length, LANES), lambda p: (0, p))
    return pl.pallas_call(
        attn_bwd_kernel,
        grid=(width // LANES,),
        in_specs=[col, col, col, col, pl.BlockSpec((2, 1, length), lambda p: (p, 0, 0)),
                  full((length, 1)), full((1, length))],
        out_specs=[col, col, col],
        out_shape=[jax.ShapeDtypeStruct((length, width), BF16)] * 3,
        scratch_shapes=[
            pltpu.VMEM((bias_rows(length), QBLOCK), F32),
            pltpu.VMEM((LANES, length), BF16),
            pltpu.VMEM((length, LANES), F32),
            pltpu.VMEM((length, LANES), F32),
        ],
        compiler_params=pltpu.CompilerParams(vmem_limit_bytes=VMEM_BYTES),
        name="attn_bwd",
    )(q, k, v, g, lse, segc, segr)


LN1_GAIN, LN1_BIAS, B_QUERY, B_VALUE, B_OUT, LN2_GAIN, LN2_BIAS, B_DOWN = range(8)


def ffn_kernel(
    x_ref, mixed_ref, cot_ref, wo_ref, wu_ref, wd_ref, vec_ref, bu_ref,
    out_ref, gh_ref, gm_ref, gwo_ref, gwu_ref, gwd_ref, gvec_ref, gbu_ref,
    h1_ref, n2_ref, n2t_ref, y_ref, gn2_ref,
):
    j = pl.program_id(0)
    last = pl.num_programs(0) - 1

    @pl.when(j == 0)
    def _():
        h1 = x_ref[...].astype(F32) + mm(mixed_ref[...], wo_ref[...], 1, 0) + vec_ref[B_OUT : B_OUT + 1, :]
        h1_ref[...] = h1
        xhat, _ = norm_parts(h1)
        n2 = xhat * vec_ref[LN2_GAIN : LN2_GAIN + 1, :] + vec_ref[LN2_BIAS : LN2_BIAS + 1, :]
        n2 = n2.astype(BF16)
        n2_ref[...] = n2
        n2t_ref[...] = n2.T

    wu = wu_ref[...]
    wd = wd_ref[...]
    cot = cot_ref[...]
    up = mm(n2_ref[...], wu, 1, 0) + bu_ref[...]
    half = 0.5 * (1.0 + lax.erf(up * 0.7071067811865476))
    act = (up * half).astype(BF16)
    slope = half + up * (jnp.exp(-0.5 * up * up) * 0.3989422804014327)
    gu = slope * mm(cot, wd, 1, 1)
    gu = gu.astype(BF16)
    gbu_ref[...] = jnp.sum(gu.astype(F32), axis=0, keepdims=True)
    gwd_ref[...] = mm(act, cot, 0, 0).astype(BF16)
    gwu_ref[...] = mm(n2t_ref[...], gu, 1, 0).astype(BF16)
    y = mm(act, wd, 1, 0)
    gn2 = mm(gu, wu, 1, 1)

    @pl.when(j == 0)
    def _():
        y_ref[...] = y
        gn2_ref[...] = gn2

    @pl.when(j != 0)
    def _():
        y_ref[...] += y
        gn2_ref[...] += gn2

    @pl.when(j == last)
    def _():
        out_ref[...] = (h1_ref[...] + (y_ref[...] + vec_ref[B_DOWN : B_DOWN + 1, :])).astype(BF16)
        xhat, rstd = norm_parts(h1_ref[...])
        gn2_all = gn2_ref[...]
        cot_f = cot_ref[...].astype(F32)
        gvec_ref[...] = jnp.zeros_like(gvec_ref)
        gvec_ref[LN2_GAIN : LN2_GAIN + 1, :] = jnp.sum(gn2_all * xhat, axis=0, keepdims=True)
        gvec_ref[LN2_BIAS : LN2_BIAS + 1, :] = jnp.sum(gn2_all, axis=0, keepdims=True)
        gvec_ref[B_DOWN : B_DOWN + 1, :] = jnp.sum(cot_f, axis=0, keepdims=True)
        gx = gn2_all * vec_ref[LN2_GAIN : LN2_GAIN + 1, :]
        mean_g = jnp.mean(gx, axis=-1, keepdims=True)
        mean_gx = jnp.mean(gx * xhat, axis=-1, keepdims=True)
        gh = cot_f + rstd * (gx - mean_g - xhat * mean_gx)
        gh_ref[...] = gh
        gb = gh.astype(BF16)
        gvec_ref[B_OUT : B_OUT + 1, :] = jnp.sum(gb.astype(F32), axis=0, keepdims=True)
        gwo_ref[...] = mm(mixed_ref[...], gb, 0, 0).astype(BF16)
        gm_ref[...] = mm(gb, wo_ref[...], 1, 1).astype(BF16)


def ffn(x, mixed, cot, wo, wu, wd, vec, bu, block=512):
    length, width = x.shape
    hidden = wu.shape[1]
    const = lambda shape: pl.BlockSpec(shape, lambda j: (0, 0), pipeline_mode=pl.Buffered(1))
    act = (length, width)
    return pl.pallas_call(
        ffn_kernel,
        grid=(hidden // block,),
        in_specs=[
            const(act), const(act), const(act), const(wo.shape),
            pl.BlockSpec((width, block), lambda j: (0, j)),
            pl.BlockSpec((block, width), lambda j: (j, 0)),
            const(vec.shape),
            pl.BlockSpec((1, block), lambda j: (0, j)),
        ],
        out_specs=[
            const(act), const(act), const(act), const(wo.shape),
            pl.BlockSpec((width, block), lambda j: (0, j)),
            pl.BlockSpec((block, width), lambda j: (j, 0)),
            const((8, width)),
            pl.BlockSpec((1, block), lambda j: (0, j)),
        ],
        out_shape=[
            jax.ShapeDtypeStruct(act, BF16),
            jax.ShapeDtypeStruct(act, F32),
            jax.ShapeDtypeStruct(act, BF16),
            jax.ShapeDtypeStruct(wo.shape, BF16),
            jax.ShapeDtypeStruct(wu.shape, BF16),
            jax.ShapeDtypeStruct(wd.shape, BF16),
            jax.ShapeDtypeStruct((8, width), F32),
            jax.ShapeDtypeStruct((1, hidden), F32),
        ],
        scratch_shapes=[
            pltpu.VMEM(act, F32),
            pltpu.VMEM(act, BF16),
            pltpu.VMEM((width, length), BF16),
            pltpu.VMEM(act, F32),
            pltpu.VMEM(act, F32),
        ],
        compiler_params=pltpu.CompilerParams(vmem_limit_bytes=VMEM_BYTES),
        name="ffn",
    )(x, mixed, cot, wo, wu, wd, vec, bu)


def qkv_bwd_kernel(
    x_ref, n1_ref, dq_ref, dk_ref, dv_ref, w_ref, gh_ref, vec_ref,
    gw_ref, gx_ref, gvec_ref, n1t_ref, acc_ref,
):
    j = pl.program_id(0)

    @pl.when(j == 0)
    def _():
        n1t_ref[...] = n1_ref[...].T
        acc_ref[...] = jnp.zeros_like(acc_ref)
        gvec_ref[...] = jnp.zeros_like(gvec_ref)

    def step(d_ref, bias_row):
        d = d_ref[...]
        gw_ref[...] = mm(n1t_ref[...], d, 1, 0).astype(BF16)
        acc_ref[...] += mm(d, w_ref[...], 1, 1)
        if bias_row is not None:
            gvec_ref[bias_row : bias_row + 1, :] = jnp.sum(d.astype(F32), axis=0, keepdims=True)

    @pl.when(j == 0)
    def _():
        step(dq_ref, B_QUERY)

    @pl.when(j == 1)
    def _():
        step(dk_ref, None)

    @pl.when(j == 2)
    def _():
        step(dv_ref, B_VALUE)
        gn1 = acc_ref[...]
        xhat, rstd = norm_parts(x_ref[...].astype(F32))
        gvec_ref[LN1_GAIN : LN1_GAIN + 1, :] = jnp.sum(gn1 * xhat, axis=0, keepdims=True)
        gvec_ref[LN1_BIAS : LN1_BIAS + 1, :] = jnp.sum(gn1, axis=0, keepdims=True)
        gx = gn1 * vec_ref[LN1_GAIN : LN1_GAIN + 1, :]
        mean_g = jnp.mean(gx, axis=-1, keepdims=True)
        mean_gx = jnp.mean(gx * xhat, axis=-1, keepdims=True)
        gx_ref[...] = gh_ref[...] + rstd * (gx - mean_g - xhat * mean_gx)


def qkv_backward(x, n1, dq, dk, dv, w_qkv, gh, vec):
    length, width = x.shape
    act = (length, width)
    const = lambda shape: pl.BlockSpec(shape, lambda j: (0, 0), pipeline_mode=pl.Buffered(1))
    return pl.pallas_call(
        qkv_bwd_kernel,
        grid=(3,),
        in_specs=[const(act)] * 5
        + [pl.BlockSpec((width, width), lambda j: (0, j)), const(act), const(vec.shape)],
        out_specs=[pl.BlockSpec((width, width), lambda j: (0, j)), const(act), const((8, width))],
        out_shape=[
            jax.ShapeDtypeStruct((width, 3 * width), BF16),
            jax.ShapeDtypeStruct(act, F32),
            jax.ShapeDtypeStruct((8, width), F32),
        ],
        scratch_shapes=[pltpu.VMEM((width, length), BF16), pltpu.VMEM(act, F32)],
        compiler_params=pltpu.CompilerParams(vmem_limit_bytes=VMEM_BYTES),
        name="qkv_bwd",
    )(x, n1, dq, dk, dv, w_qkv, gh, vec)


def gather(v):
    return lax.all_gather(v, AXES, axis=0, tiled=True)


def scatter(v):
    return lax.psum_scatter(v, AXES, scatter_dimension=0, tiled=True)


def shards(
    inputs, segment_ids, cotangent, ln1_gain, ln1_bias, w_query, b_query, w_key, w_value, b_value,
    w_out, b_out, ln2_gain, ln2_bias, w_up, b_up, w_down, b_down,
):
    own, width = w_query.shape
    length = inputs.shape[0]
    low = lambda v: v.astype(BF16)
    table = jnp.stack(
        [low(v) for v in (ln1_gain, ln1_bias, b_query, b_value, b_out, ln2_gain, ln2_bias, b_down)], 1
    )
    table = jnp.concatenate([table, low(b_up).reshape(own, -1)], 1)
    table = jnp.pad(table, ((0, 0), (0, LANES - table.shape[1])))
    first = gather(jnp.concatenate([low(w_query), low(w_key), low(w_value), table], 1))
    wo = gather(low(w_out))
    wu = gather(low(w_up))
    wd = gather(low(w_down))
    extra = first[:, 3 * width :].astype(F32)
    vec = extra[:, :8].T
    bu = extra[:, 8 : 8 + w_up.shape[1] // width].reshape(1, -1)
    segc = segment_ids.reshape(length, 1)
    q, k, v, mixed, lse, n1 = attention_forward(inputs, first, vec, segc, segment_ids)
    out, gh, gm, gwo, gwu, gwd, gvec_a, gbu = ffn(inputs, mixed, cotangent, wo, wu, wd, vec, bu)
    dq, dk, dv = attention_backward(q, k, v, gm, lse, segc, segment_ids)
    gw, gx, gvec_b = qkv_backward(inputs, n1, dq, dk, dv, first, gh, vec)
    gtab = jnp.concatenate([(gvec_a + gvec_b).T, gbu.reshape(width, -1)], 1)
    gtab = jnp.pad(gtab, ((0, 0), (0, LANES - gtab.shape[1])))
    s_o = scatter(gwo).astype(F32)
    s_u = scatter(gwu).astype(F32)
    s_d = scatter(gwd).astype(F32)
    s_q = scatter(jnp.concatenate([gw, gtab.astype(BF16)], 1)).astype(F32)
    tab = s_q[:, 3 * width :]
    g1, b1, bq, bv, bo, g2, b2, bd = (tab[:, r] for r in range(8))
    return (
        out, gx, g1, b1, s_q[:, :width], bq, s_q[:, width : 2 * width], s_q[:, 2 * width : 3 * width],
        bv, s_o, bo, g2, b2, s_u, tab[:, 8 : 8 + w_up.shape[1] // width].reshape(-1), s_d, bd,
    )


def solution(mesh):
    row, vec = P(AXES, None), P(AXES)
    weights = (vec, vec, row, vec, row, row, vec, row, vec, vec, vec, row, vec, row, vec)
    return jax.shard_map(
        shards,
        mesh=mesh,
        in_specs=(row, row, row) + weights,
        out_specs=(row, row) + weights,
        check_vma=False,
    )
```
